32 devices in a mesh: pr: 8 (over y, x, core), pc: 4 (over z).
Axes of the slice: x: 2, y: 2, z: 4, core: 2. Of those that a mesh axis runs over, the one named last changes fastest.
Arguments:
- pair_array: bfloat16 [256, 256, 128], P('pr', 'pc'), may hold values from -6 to 6
- left_weight: bfloat16 [128, 128], replicated, may hold values from -0.5 to 0.5
- right_weight: bfloat16 [128, 128], replicated, may hold values from -0.5 to 0.5
- left_gate: bfloat16 [128, 128], replicated, may hold values from -0.5 to 0.5
- right_gate: bfloat16 [128, 128], replicated, may hold values from -0.5 to 0.5
- mid_gain: float32 [128], replicated, may hold values from 0.25 to 1.75
- out_weight: bfloat16 [128, 128], replicated, may hold values from -0.5 to 0.5
- out_gate: bfloat16 [128, 128], replicated, may hold values from -0.5 to 0.5
Outputs:
- pair_update: bfloat16 [256, 256, 128], P('pr', 'pc')
The draws below stay inside these ranges and needn't reach their ends.
All inputs are finite; a program needn't handle non-finite values.
Results may differ from the reference program's by a relative error of at most 0.012.
Values may be sent and summed in bfloat16 or wider, within the bound.
A program may use at most 128 MiB of HBM per device.

```python
import jax
import jax.numpy as jnp
from jax import lax

RESIDUES = 256
PAIR_WIDTH = 128
MIX_WIDTH = 128


def shard_levels(rng, extent, pieces, least, largest):
    loudness = 1.0
    for axis_at, parts in pieces:
        draws = jax.random.uniform(jax.random.fold_in(jax.random.fold_in(rng, 6), axis_at), (parts,), jnp.float32, least / len(pieces), largest / len(pieces))
        loudness = loudness * jnp.repeat(jnp.exp(draws), extent[axis_at] // parts).reshape((-1,) + (1,) * (len(extent) - 1 - axis_at))
    return loudness


def bell_draw(key, shape, scale, reach, pieces=(), dtype=jnp.bfloat16):
    entries = jax.random.normal(key, shape, jnp.float32) * scale
    if len(pieces) > 0:
        entries = shard_levels(key, shape, pieces, -0.22, 0.18) * entries
    return jnp.clip(entries, min=-reach, max=reach).astype(dtype)


def setup_inputs(seed: int = 0) -> dict:
    keys = jax.random.split(jax.random.key(seed), 9)
    pair_array = bell_draw(keys[0], (RESIDUES, RESIDUES, PAIR_WIDTH), 1.0, 6.0, ((0, 8), (1, 4)))
    left_weight = bell_draw(keys[1], (PAIR_WIDTH, MIX_WIDTH), PAIR_WIDTH ** -0.5, 0.5)
    right_weight = bell_draw(keys[2], (PAIR_WIDTH, MIX_WIDTH), PAIR_WIDTH ** -0.5, 0.5)
    left_gate = bell_draw(keys[3], (PAIR_WIDTH, MIX_WIDTH), PAIR_WIDTH ** -0.5, 0.5)
    right_gate = bell_draw(keys[4], (PAIR_WIDTH, MIX_WIDTH), PAIR_WIDTH ** -0.5, 0.5)
    mid_gain = jnp.clip(1.0 + 0.15 * jax.random.normal(keys[5], (MIX_WIDTH,), jnp.float32), 0.25, 1.75)
    out_weight = bell_draw(keys[6], (MIX_WIDTH, PAIR_WIDTH), MIX_WIDTH ** -0.5, 0.5)
    out_gate = bell_draw(keys[7], (PAIR_WIDTH, PAIR_WIDTH), PAIR_WIDTH ** -0.5, 0.5)
    return {"pair_array": pair_array, "left_weight": left_weight, "right_weight": right_weight, "left_gate": left_gate, "right_gate": right_gate, "mid_gain": mid_gain, "out_weight": out_weight, "out_gate": out_gate}


def unit_channels(values, channel_gain):
    centred = values - lax.optimization_barrier(jnp.mean(values, axis=-1, keepdims=True))
    return centred * lax.rsqrt(lax.optimization_barrier(jnp.mean(centred * centred, axis=-1, keepdims=True)) + 1e-05) * channel_gain

def make_factors(pair_in, left_weight, right_weight, left_gate, right_gate):
    ready = pair_in
    left = jnp.einsum('ijc,cd->ijd', ready.astype(jnp.float32), left_weight.astype(jnp.float32))
    left = left * jax.nn.sigmoid(jnp.einsum('ijc,cd->ijd', ready.astype(jnp.float32), left_gate.astype(jnp.float32)))
    right = jnp.einsum('ijc,cd->ijd', ready.astype(jnp.float32), right_weight.astype(jnp.float32))
    right = right * jax.nn.sigmoid(jnp.einsum('ijc,cd->ijd', ready.astype(jnp.float32), right_gate.astype(jnp.float32)))
    return (ready, left.astype(jnp.bfloat16), right.astype(jnp.bfloat16))

def to_pair(mixed, ready, mid_gain, out_weight, out_gate):
    scaled = unit_channels(mixed.astype(jnp.float32), mid_gain).astype(jnp.bfloat16)
    scaled = lax.optimization_barrier(scaled)
    gate = jax.nn.sigmoid(jnp.einsum('ijc,cd->ijd', ready.astype(jnp.float32), out_gate.astype(jnp.float32)))
    return (jnp.einsum('ijd,dc->ijc', scaled.astype(jnp.float32), out_weight.astype(jnp.float32)) * gate).astype(jnp.bfloat16)

def reference(pair_array, left_weight, right_weight, left_gate, right_gate, mid_gain, out_weight, out_gate):
    ready, left, right = make_factors(pair_array, left_weight, right_weight, left_gate, right_gate)
    left, right = lax.optimization_barrier((left, right))

    def one_channel(pair_of):
        return (jnp.dot(pair_of[0].T, pair_of[1], preferred_element_type=jnp.float32) * RESIDUES ** (-0.5)).astype(jnp.bfloat16)
    mixed = jnp.moveaxis(lax.map(one_channel, (jnp.moveaxis(left, -1, 0), jnp.moveaxis(right, -1, 0))), 0, -1)
    mixed = lax.optimization_barrier(mixed)
    return to_pair(mixed, ready, mid_gain, out_weight, out_gate)
```

```python
import functools

import jax
import jax.numpy as jnp
from jax import lax
from jax.experimental import pallas as pl
from jax.experimental.pallas import tpu as pltpu
from jax.sharding import PartitionSpec as P

MESH = pl.DeviceIdType.MESH
BF16 = jnp.bfloat16
F32 = jnp.float32
LANES = 128
SUB = 16


def unit_channels(values, channel_gain):
    centred = values - jnp.mean(values, axis=-1, keepdims=True)
    return (
        centred
        * lax.rsqrt(jnp.mean(centred * centred, axis=-1, keepdims=True) + 1e-05)
        * channel_gain
    )


def make_factors(pair_in, left_weight, right_weight, left_gate, right_gate):
    left = jnp.einsum("ijc,cd->ijd", pair_in, left_weight, preferred_element_type=F32)
    left = left * jax.nn.sigmoid(
        jnp.einsum("ijc,cd->ijd", pair_in, left_gate, preferred_element_type=F32)
    )
    right = jnp.einsum("ijc,cd->ijd", pair_in, right_weight, preferred_element_type=F32)
    right = right * jax.nn.sigmoid(
        jnp.einsum("ijc,cd->ijd", pair_in, right_gate, preferred_element_type=F32)
    )
    return (pair_in, left.astype(BF16), right.astype(BF16))


def to_pair(mixed, ready, mid_gain, out_weight, out_gate):
    scaled = unit_channels(mixed.astype(F32), mid_gain).astype(BF16)
    scaled = lax.optimization_barrier(scaled)
    gate = jax.nn.sigmoid(jnp.einsum("ijc,cd->ijd", ready, out_gate, preferred_element_type=F32))
    return (
        jnp.einsum("ijd,dc->ijc", scaled, out_weight, preferred_element_type=F32) * gate
    ).astype(BF16)


def plain(
    pair_array, left_weight, right_weight, left_gate, right_gate, mid_gain, out_weight, out_gate
):
    ready, left, right = make_factors(pair_array, left_weight, right_weight, left_gate, right_gate)
    count = pair_array.shape[0] * lax.axis_size("pr")
    left_lines, right_lines = (
        lax.all_to_all(left, "pr", split_axis=2, concat_axis=0, tiled=True),
        lax.all_to_all(right, "pr", split_axis=2, concat_axis=0, tiled=True),
    )
    strip = jnp.einsum(
        "kid,kjd->ijd",
        lax.all_gather(left_lines, "pc", axis=1, tiled=True),
        right_lines,
        preferred_element_type=F32,
    )
    strip = (strip * count ** (-0.5)).astype(BF16)
    mixed = lax.all_to_all(strip, "pr", split_axis=0, concat_axis=2, tiled=True)
    return to_pair(mixed, ready, mid_gain, out_weight, out_gate)


def nt(a, b):
    return lax.dot_general(a, b, (((1,), (1,)), ((), ())), preferred_element_type=F32)


def tn(a, b):
    return lax.dot_general(a, b, (((0,), (0,)), ((), ())), preferred_element_type=F32)


GROUPS = ((0, 0), (0, 1), (1, 0), (1, 1))


def kernel(
    n_p, n_q, x_ref, lw_ref, rw_ref, lg_ref, rg_ref, gain_ref, ow_ref, og_ref, out_ref,
    turn, lsend, rsend, lrecv, rrecv, osend, orecv, gate,
    l_ss, l_rs, r_ss, r_rs, o_ss, o_rs,
):
    p = lax.axis_index("pr")
    q = lax.axis_index("pc")
    zh = q // 2
    zl = q % 2
    me = p * 2 + zl
    n_e = n_p * 2
    per = lsend.shape[1] // SUB
    width = x_ref.shape[1]
    rows = x_ref.shape[0] // 2
    channels = n_e * per
    count = n_p * x_ref.shape[0]

    barrier = pltpu.get_barrier_semaphore()
    for dp in range(n_p):
        for dh, dl in GROUPS:
            if (dp, dh, dl) != (0, 0, 0):
                to = (lax.rem(p + dp, n_p), lax.rem(zh + dh, 2) * 2 + lax.rem(zl + dl, 2))
                pl.semaphore_signal(barrier, inc=1, device_id=to, device_id_type=MESH)

    def pair_rows(k):
        return jnp.concatenate([x_ref[k], x_ref[k + rows]], axis=0)

    def factor(w_ref, g_ref, send):
        both = jnp.concatenate([w_ref[...].T, g_ref[...].T], axis=0)

        def step(k, _):
            pr = nt(both, pair_rows(k))
            turn[pl.ds(k, channels, stride=SUB), :] = pr[:channels] * jax.nn.sigmoid(pr[channels:])
            return 0

        lax.fori_loop(0, rows, step, 0, unroll=2)

        def cast(e, _):
            at = pl.multiple_of(e * per * SUB, per * SUB)
            send[e] = turn[pl.ds(at, per * SUB), :].astype(BF16)
            return 0

        lax.fori_loop(0, n_e, cast, 0)

    def r_copy(dp, dl, arriving=False):
        to_p, to_l = lax.rem(p + dp, n_p), lax.rem(zl + dl, 2)
        return pltpu.make_async_remote_copy(
            src_ref=rsend.at[to_p * 2 + to_l],
            dst_ref=rrecv.at[dl, dp],
            send_sem=r_ss.at[dl, dp],
            recv_sem=r_rs.at[dl, dp],
            device_id=(to_p, zh * 2 + to_l),
            device_id_type=MESH,
        )

    def l_copy(dp, group):
        dh, dl = GROUPS[group]
        to_p, to_l = lax.rem(p + dp, n_p), lax.rem(zl + dl, 2)
        return pltpu.make_async_remote_copy(
            src_ref=lsend.at[to_p * 2 + to_l],
            dst_ref=lrecv.at[group, dp],
            send_sem=l_ss.at[group, dp],
            recv_sem=l_rs.at[group, dp],
            device_id=(to_p, lax.rem(zh + dh, 2) * 2 + to_l),
            device_id_type=MESH,
        )

    factor(rw_ref, rg_ref, rsend)
    pl.semaphore_wait(barrier, n_p * n_q - 1)
    for dl in (1, 0):
        for dp in range(n_p):
            if (dp, dl) != (0, 0):
                r_copy(dp, dl).start()
    factor(lw_ref, lg_ref, lsend)
    for group in range(4):
        for dp in range(n_p):
            if (dp, group) != (0, 0):
                l_copy(dp, group).start()
    rrecv[0, 0] = rsend[me]
    lrecv[0, 0] = lsend[me]

    def make_gate(k, _):
        gate[k] = jax.nn.sigmoid(
            jnp.dot(pair_rows(k), og_ref[...], preferred_element_type=F32)
        )
        return 0

    lax.fori_loop(0, rows, make_gate, 0)

    for dl in (1, 0):
        for dp in range(n_p):
            if (dp, dl) != (0, 0):
                r_copy(dp, dl).wait_recv()

    low = lax.broadcasted_iota(jnp.int32, (SUB, LANES), 1) < width

    def o_copy(group, b, dl):
        dh, gl = GROUPS[group]
        z = lax.rem(zh + dh, 2) * 2 + lax.rem(zl + gl, 2)
        to_p, to_l = z * 2 + b, lax.rem(zl + dl, 2)
        away = (to_p != p) if dl == 0 else None
        return away, pltpu.make_async_remote_copy(
            src_ref=osend.at[group, b, dl],
            dst_ref=orecv.at[me],
            send_sem=o_ss.at[group, b, dl],
            recv_sem=o_rs.at[me],
            device_id=(to_p, zh * 2 + to_l),
            device_id_type=MESH,
        )

    for group in range(4):
        for dp in range(n_p):
            if (dp, group) != (0, 0):
                l_copy(dp, group).wait_recv()

        def products(d, _):
            at = pl.ds(pl.multiple_of(d * SUB, SUB), SUB)
            left = lrecv[group, :, at, :].reshape(n_p * SUB, LANES)
            for dl in range(2):
                right = rrecv[dl, :, at, :].reshape(n_p * SUB, LANES)
                acc = tn(left, right)
                for b in range(2):
                    top = b * 2 * SUB
                    a0, c0 = acc[top : top + SUB], acc[top + SUB : top + 2 * SUB]
                    b0 = acc[width + top : width + top + SUB]
                    d0 = acc[width + top + SUB : width + top + 2 * SUB]
                    tile = jnp.where(low, a0, d0) + pltpu.roll(
                        jnp.where(low, c0, b0), width, 1
                    )
                    osend[group, b, dl, at, :] = (tile * count ** (-0.5)).astype(BF16)
            return 0

        lax.fori_loop(0, per, products, 0, unroll=2)
        for b in range(2):
            for dl in (1, 0):
                away, copy = o_copy(group, b, dl)
                if away is None:
                    copy.start()
                else:

                    @pl.when(away)
                    def _():
                        copy.start()

                    @pl.when(jnp.logical_not(away))
                    def _():
                        orecv[me] = osend[group, b, dl]

    gain = jnp.broadcast_to(gain_ref[...], (channels, channels)).T
    for off in range(1, n_e):
        at = lax.rem(me + off, n_e)
        pltpu.make_async_remote_copy(
            src_ref=osend.at[0, 0, 0],
            dst_ref=orecv.at[at],
            send_sem=o_ss.at[0, 0, 0],
            recv_sem=o_rs.at[at],
            device_id=(p, q),
            device_id_type=MESH,
        ).wait_recv()

    def widen(e, _):
        at = pl.multiple_of(e * per * SUB, per * SUB)
        turn[pl.ds(at, per * SUB), :] = orecv[e].astype(F32)
        return 0

    lax.fori_loop(0, n_e, widen, 0)

    def finish(k, _):
        v = turn[pl.ds(k, channels, stride=SUB), :]
        v = v - jnp.mean(v, axis=0, keepdims=True)
        v = v * lax.rsqrt(jnp.mean(v * v, axis=0, keepdims=True) + 1e-05) * gain
        res = (tn(v.astype(BF16), ow_ref[...]) * gate[k]).astype(BF16)
        out_ref[k] = res[:width]
        out_ref[k + rows] = res[width:]
        return 0

    lax.fori_loop(0, rows, finish, 0, unroll=2)

    for dl in range(2):
        for dp in range(n_p):
            if (dp, dl) != (0, 0):
                r_copy(dp, dl).wait_send()
    for group in range(4):
        for dp in range(n_p):
            if (dp, group) != (0, 0):
                l_copy(dp, group).wait_send()
        for b in range(2):
            for dl in range(2):
                away, copy = o_copy(group, b, dl)
                if away is None:
                    copy.wait_send()
                else:

                    @pl.when(away)
                    def _():
                        copy.wait_send()


def fused(n_p, n_q, pair_array, lw, rw, lg, rg, gain, ow, og):
    channels = lw.shape[1]
    n_e = n_p * 2
    slab = channels // n_e * SUB
    rows = pair_array.shape[0] // 2
    dma = pltpu.SemaphoreType.DMA
    return pl.pallas_call(
        functools.partial(kernel, n_p, n_q),
        out_shape=jax.ShapeDtypeStruct(pair_array.shape, BF16),
        in_specs=[pl.BlockSpec(memory_space=pltpu.VMEM)] * 8,
        out_specs=pl.BlockSpec(memory_space=pltpu.VMEM),
        scratch_shapes=[
            pltpu.VMEM((channels * SUB, LANES), F32),
            pltpu.VMEM((n_e, slab, LANES), BF16),
            pltpu.VMEM((n_e, slab, LANES), BF16),
            pltpu.VMEM((4, n_p, slab, LANES), BF16),
            pltpu.VMEM((2, n_p, slab, LANES), BF16),
            pltpu.VMEM((4, 2, 2, slab, LANES), BF16),
            pltpu.VMEM((n_e, slab, LANES), BF16),
            pltpu.VMEM((rows, LANES, channels), F32),
            dma((4, n_p)),
            dma((4, n_p)),
            dma((2, n_p)),
            dma((2, n_p)),
            dma((4, 2, 2)),
            dma((n_e,)),
        ],
        compiler_params=pltpu.CompilerParams(
            collective_id=0, has_side_effects=True, vmem_limit_bytes=40 * 2**20
        ),
    )(pair_array, lw, rw, lg, rg, gain.reshape(1, channels), ow, og)


def solution(mesh):
    n_p, n_q = mesh.shape["pr"], mesh.shape["pc"]

    def on_device(pair_array, lw, *rest):
        first, second, wide = pair_array.shape
        fits = (
            n_q == 4
            and first == 2 * SUB
            and second == 2 * first
            and n_p == 2 * n_q
            and 2 * second == LANES
            and wide == LANES
            and lw.shape[1] == LANES
        )
        if fits:
            return fused(n_p, n_q, pair_array, lw, *rest)
        return plain(pair_array, lw, *rest)

    return jax.shard_map(
        on_device,
        mesh=mesh,
        in_specs=(P("pr", "pc", None), P(), P(), P(), P(), P(), P(), P()),
        out_specs=P("pr", "pc", None),
        check_vma=False,
    )
```

```python
import functools

import jax
import jax.numpy as jnp
from jax import lax
from jax.experimental import pallas as pl
from jax.experimental.pallas import tpu as pltpu
from jax.sharding import PartitionSpec as P

MESH = pl.DeviceIdType.MESH
BF16 = jnp.bfloat16
F32 = jnp.float32
LANES = 128
SUB = 16
UF, UP, UE = 16, 8, 16


def unit_channels(values, channel_gain):
    centred = values - jnp.mean(values, axis=-1, keepdims=True)
    return (
        centred
        * lax.rsqrt(jnp.mean(centred * centred, axis=-1, keepdims=True) + 1e-05)
        * channel_gain
    )


def make_factors(pair_in, left_weight, right_weight, left_gate, right_gate):
    left = jnp.einsum("ijc,cd->ijd", pair_in, left_weight, preferred_element_type=F32)
    left = left * jax.nn.sigmoid(
        jnp.einsum("ijc,cd->ijd", pair_in, left_gate, preferred_element_type=F32)
    )
    right = jnp.einsum("ijc,cd->ijd", pair_in, right_weight, preferred_element_type=F32)
    right = right * jax.nn.sigmoid(
        jnp.einsum("ijc,cd->ijd", pair_in, right_gate, preferred_element_type=F32)
    )
    return (pair_in, left.astype(BF16), right.astype(BF16))


def to_pair(mixed, ready, mid_gain, out_weight, out_gate):
    scaled = unit_channels(mixed.astype(F32), mid_gain).astype(BF16)
    scaled = lax.optimization_barrier(scaled)
    gate = jax.nn.sigmoid(jnp.einsum("ijc,cd->ijd", ready, out_gate, preferred_element_type=F32))
    return (
        jnp.einsum("ijd,dc->ijc", scaled, out_weight, preferred_element_type=F32) * gate
    ).astype(BF16)


def plain(
    pair_array, left_weight, right_weight, left_gate, right_gate, mid_gain, out_weight, out_gate
):
    ready, left, right = make_factors(pair_array, left_weight, right_weight, left_gate, right_gate)
    count = pair_array.shape[0] * lax.axis_size("pr")
    left_lines, right_lines = (
        lax.all_to_all(left, "pr", split_axis=2, concat_axis=0, tiled=True),
        lax.all_to_all(right, "pr", split_axis=2, concat_axis=0, tiled=True),
    )
    strip = jnp.einsum(
        "kid,kjd->ijd",
        lax.all_gather(left_lines, "pc", axis=1, tiled=True),
        right_lines,
        preferred_element_type=F32,
    )
    strip = (strip * count ** (-0.5)).astype(BF16)
    mixed = lax.all_to_all(strip, "pr", split_axis=0, concat_axis=2, tiled=True)
    return to_pair(mixed, ready, mid_gain, out_weight, out_gate)


def nt(a, b):
    return lax.dot_general(a, b, (((1,), (1,)), ((), ())), preferred_element_type=F32)


def tn(a, b):
    return lax.dot_general(a, b, (((0,), (0,)), ((), ())), preferred_element_type=F32)


GROUPS = ((0, 0), (0, 1), (1, 0), (1, 1))


def kernel(
    n_p, n_q, x_hbm, lw_hbm, rw_hbm, lg_hbm, rg_hbm, gain_hbm, ow_hbm, og_hbm, out_ref,
    x_ref, lw_ref, rw_ref, lg_ref, rg_ref, gain_ref, ow_ref, og_ref, in_s,
    turn, lsend, rsend, lrecv, rrecv, osend, orecv, gate,
    l_ss, l_rs, r_ss, r_rs, o_ss, o_rs,
):
    p = lax.axis_index("pr")
    q = lax.axis_index("pc")
    zh = q // 2
    zl = q % 2
    me = p * 2 + zl
    n_e = n_p * 2
    per = lsend.shape[1] // SUB
    width = x_ref.shape[1]
    rows = x_ref.shape[0] // 2
    channels = n_e * per
    count = n_p * x_ref.shape[0]

    brought = [
        pltpu.make_async_copy(src, dst, in_s.at[at])
        for at, (src, dst) in enumerate(
            (
                (x_hbm, x_ref), (rw_hbm, rw_ref), (rg_hbm, rg_ref), (lw_hbm, lw_ref),
                (lg_hbm, lg_ref), (og_hbm, og_ref), (ow_hbm, ow_ref), (gain_hbm, gain_ref),
            )
        )
    ]
    for copy in brought:
        copy.start()

    barrier = pltpu.get_barrier_semaphore()
    for dp in range(n_p):
        for dh, dl in GROUPS:
            if (dp, dh, dl) != (0, 0, 0):
                to = (lax.rem(p + dp, n_p), lax.rem(zh + dh, 2) * 2 + lax.rem(zl + dl, 2))
                pl.semaphore_signal(barrier, inc=1, device_id=to, device_id_type=MESH)

    def pair_rows(k):
        return jnp.concatenate([x_ref[k], x_ref[k + rows]], axis=0)

    def factor(w_ref, g_ref, send):
        both = jnp.concatenate([w_ref[...].T, g_ref[...].T], axis=0)

        def step(k, _):
            pr = nt(both, pair_rows(k))
            turn[pl.ds(k, channels, stride=SUB), :] = pr[:channels] * jax.nn.sigmoid(pr[channels:])
            return 0

        lax.fori_loop(0, rows, step, 0, unroll=UF)

        def cast(e, _):
            at = pl.multiple_of(e * per * SUB, per * SUB)
            send[e] = turn[pl.ds(at, per * SUB), :].astype(BF16)
            return 0

        lax.fori_loop(0, n_e, cast, 0, unroll=4)

    def r_copy(dp, dl, arriving=False):
        to_p, to_l = lax.rem(p + dp, n_p), lax.rem(zl + dl, 2)
        return pltpu.make_async_remote_copy(
            src_ref=rsend.at[to_p * 2 + to_l],
            dst_ref=rrecv.at[dl, dp],
            send_sem=r_ss.at[dl, dp],
            recv_sem=r_rs.at[dl, dp],
            device_id=(to_p, zh * 2 + to_l),
            device_id_type=MESH,
        )

    def l_copy(dp, group):
        dh, dl = GROUPS[group]
        to_p, to_l = lax.rem(p + dp, n_p), lax.rem(zl + dl, 2)
        return pltpu.make_async_remote_copy(
            src_ref=lsend.at[to_p * 2 + to_l],
            dst_ref=lrecv.at[group, dp],
            send_sem=l_ss.at[group, dp],
            recv_sem=l_rs.at[group, dp],
            device_id=(to_p, lax.rem(zh + dh, 2) * 2 + to_l),
            device_id_type=MESH,
        )

    for copy in brought:
        copy.wait()
    factor(rw_ref, rg_ref, rsend)
    pl.semaphore_wait(barrier, n_p * n_q - 1)
    for dl in (1, 0):
        for dp in range(n_p):
            if (dp, dl) != (0, 0):
                r_copy(dp, dl).start()
    factor(lw_ref, lg_ref, lsend)
    for group in range(4):
        for dp in range(n_p):
            if (dp, group) != (0, 0):
                l_copy(dp, group).start()
    rrecv[0, 0] = rsend[me]
    lrecv[0, 0] = lsend[me]

    def make_gate(k, _):
        gate[k] = jax.nn.sigmoid(
            jnp.dot(pair_rows(k), og_ref[...], preferred_element_type=F32)
        )
        return 0

    lax.fori_loop(0, rows, make_gate, 0, unroll=4)

    for dl in (1, 0):
        for dp in range(n_p):
            if (dp, dl) != (0, 0):
                r_copy(dp, dl).wait_recv()

    low = lax.broadcasted_iota(jnp.int32, (SUB, LANES), 1) < width

    def o_copy(group, b, dl):
        dh, gl = GROUPS[group]
        z = lax.rem(zh + dh, 2) * 2 + lax.rem(zl + gl, 2)
        to_p, to_l = z * 2 + b, lax.rem(zl + dl, 2)
        away = (to_p != p) if dl == 0 else None
        return away, pltpu.make_async_remote_copy(
            src_ref=osend.at[group, b, dl],
            dst_ref=orecv.at[me],
            send_sem=o_ss.at[group, b, dl],
            recv_sem=o_rs.at[me],
            device_id=(to_p, zh * 2 + to_l),
            device_id_type=MESH,
        )

    for group in range(4):
        for dp in range(n_p):
            if (dp, group) != (0, 0):
                l_copy(dp, group).wait_recv()

        def products(d, _):
            at = pl.ds(pl.multiple_of(d * SUB, SUB), SUB)
            left = lrecv[group, :, at, :].reshape(n_p * SUB, LANES)
            right = [rrecv[dl, :, at, :].reshape(n_p * SUB, LANES) for dl in range(2)]
            sums = tn(left, jnp.concatenate(right, axis=1))
            for dl in range(2):
                acc = sums[:, dl * LANES : (dl + 1) * LANES]
                for b in range(2):
                    top = b * 2 * SUB
                    a0, c0 = acc[top : top + SUB], acc[top + SUB : top + 2 * SUB]
                    b0 = acc[width + top : width + top + SUB]
                    d0 = acc[width + top + SUB : width + top + 2 * SUB]
                    tile = jnp.where(low, a0, d0) + pltpu.roll(
                        jnp.where(low, c0, b0), width, 1
                    )
                    osend[group, b, dl, at, :] = (tile * count ** (-0.5)).astype(BF16)
            return 0

        lax.fori_loop(0, per, products, 0, unroll=UP)
        for b in range(2):
            for dl in (1, 0):
                away, copy = o_copy(group, b, dl)
                if away is None:
                    copy.start()
                else:

                    @pl.when(away)
                    def _():
                        copy.start()

                    @pl.when(jnp.logical_not(away))
                    def _():
                        orecv[me] = osend[group, b, dl]

    gain = jnp.broadcast_to(gain_ref[...], (channels, channels)).T
    for off in range(1, n_e):
        at = lax.rem(me + off, n_e)
        pltpu.make_async_remote_copy(
            src_ref=osend.at[0, 0, 0],
            dst_ref=orecv.at[at],
            send_sem=o_ss.at[0, 0, 0],
            recv_sem=o_rs.at[at],
            device_id=(p, q),
            device_id_type=MESH,
        ).wait_recv()

    def widen(e, _):
        at = pl.multiple_of(e * per * SUB, per * SUB)
        turn[pl.ds(at, per * SUB), :] = orecv[e].astype(F32)
        return 0

    lax.fori_loop(0, n_e, widen, 0, unroll=4)

    def finish(k, _):
        v = turn[pl.ds(k, channels, stride=SUB), :]
        v = v - jnp.mean(v, axis=0, keepdims=True)
        v = v * lax.rsqrt(jnp.mean(v * v, axis=0, keepdims=True) + 1e-05) * gain
        res = (tn(v.astype(BF16), ow_ref[...]) * gate[k]).astype(BF16)
        out_ref[k] = res[:width]
        out_ref[k + rows] = res[width:]
        return 0

    lax.fori_loop(0, rows, finish, 0, unroll=UE)

    for dl in range(2):
        for dp in range(n_p):
            if (dp, dl) != (0, 0):
                r_copy(dp, dl).wait_send()
    for group in range(4):
        for dp in range(n_p):
            if (dp, group) != (0, 0):
                l_copy(dp, group).wait_send()
        for b in range(2):
            for dl in range(2):
                away, copy = o_copy(group, b, dl)
                if away is None:
                    copy.wait_send()
                else:

                    @pl.when(away)
                    def _():
                        copy.wait_send()


def fused(n_p, n_q, pair_array, lw, rw, lg, rg, gain, ow, og):
    channels = lw.shape[1]
    n_e = n_p * 2
    slab = channels // n_e * SUB
    rows = pair_array.shape[0] // 2
    dma = pltpu.SemaphoreType.DMA
    return pl.pallas_call(
        functools.partial(kernel, n_p, n_q),
        out_shape=jax.ShapeDtypeStruct(pair_array.shape, BF16),
        in_specs=[pl.BlockSpec(memory_space=pltpu.HBM)] * 8,
        out_specs=pl.BlockSpec(memory_space=pltpu.VMEM),
        scratch_shapes=[
            pltpu.VMEM(pair_array.shape, BF16),
            *[pltpu.VMEM(lw.shape, BF16)] * 4,
            pltpu.VMEM((1, channels), F32),
            pltpu.VMEM(ow.shape, BF16),
            pltpu.VMEM(og.shape, BF16),
            dma((8,)),
            pltpu.VMEM((channels * SUB, LANES), F32),
            pltpu.VMEM((n_e, slab, LANES), BF16),
            pltpu.VMEM((n_e, slab, LANES), BF16),
            pltpu.VMEM((4, n_p, slab, LANES), BF16),
            pltpu.VMEM((2, n_p, slab, LANES), BF16),
            pltpu.VMEM((4, 2, 2, slab, LANES), BF16),
            pltpu.VMEM((n_e, slab, LANES), BF16),
            pltpu.VMEM((rows, LANES, channels), F32),
            dma((4, n_p)),
            dma((4, n_p)),
            dma((2, n_p)),
            dma((2, n_p)),
            dma((4, 2, 2)),
            dma((n_e,)),
        ],
        compiler_params=pltpu.CompilerParams(
            collective_id=0, has_side_effects=True, vmem_limit_bytes=67_043_328
        ),
    )(pair_array, lw, rw, lg, rg, gain.reshape(1, channels), ow, og)


def solution(mesh):
    n_p, n_q = mesh.shape["pr"], mesh.shape["pc"]

    def on_device(pair_array, lw, *rest):
        first, second, wide = pair_array.shape
        fits = (
            n_q == 4
            and first == 2 * SUB
            and second == 2 * first
            and n_p == 2 * n_q
            and 2 * second == LANES
            and wide == LANES
            and lw.shape[1] == LANES
        )
        if fits:
            return fused(n_p, n_q, pair_array, lw, *rest)
        return plain(pair_array, lw, *rest)

    return jax.shard_map(
        on_device,
        mesh=mesh,
        in_specs=(P("pr", "pc", None), P(), P(), P(), P(), P(), P(), P()),
        out_specs=P("pr", "pc", None),
        check_vma=False,
    )
```

```python
import functools

import jax
import jax.numpy as jnp
from jax import lax
from jax.experimental import pallas as pl
from jax.experimental.pallas import tpu as pltpu
from jax.sharding import PartitionSpec as P

MESH = pl.DeviceIdType.MESH
BF16 = jnp.bfloat16
F32 = jnp.float32
LANES = 128
SUB = 16
UF, UP, UE = 16, 8, 16


def unit_channels(values, channel_gain):
    centred = values - jnp.mean(values, axis=-1, keepdims=True)
    return (
        centred
        * lax.rsqrt(jnp.mean(centred * centred, axis=-1, keepdims=True) + 1e-05)
        * channel_gain
    )


def make_factors(pair_in, left_weight, right_weight, left_gate, right_gate):
    left = jnp.einsum("ijc,cd->ijd", pair_in, left_weight, preferred_element_type=F32)
    left = left * jax.nn.sigmoid(
        jnp.einsum("ijc,cd->ijd", pair_in, left_gate, preferred_element_type=F32)
    )
    right = jnp.einsum("ijc,cd->ijd", pair_in, right_weight, preferred_element_type=F32)
    right = right * jax.nn.sigmoid(
        jnp.einsum("ijc,cd->ijd", pair_in, right_gate, preferred_element_type=F32)
    )
    return (pair_in, left.astype(BF16), right.astype(BF16))


def to_pair(mixed, ready, mid_gain, out_weight, out_gate):
    scaled = unit_channels(mixed.astype(F32), mid_gain).astype(BF16)
    scaled = lax.optimization_barrier(scaled)
    gate = jax.nn.sigmoid(jnp.einsum("ijc,cd->ijd", ready, out_gate, preferred_element_type=F32))
    return (
        jnp.einsum("ijd,dc->ijc", scaled, out_weight, preferred_element_type=F32) * gate
    ).astype(BF16)


def plain(
    pair_array, left_weight, right_weight, left_gate, right_gate, mid_gain, out_weight, out_gate
):
    ready, left, right = make_factors(pair_array, left_weight, right_weight, left_gate, right_gate)
    count = pair_array.shape[0] * lax.axis_size("pr")
    left_lines, right_lines = (
        lax.all_to_all(left, "pr", split_axis=2, concat_axis=0, tiled=True),
        lax.all_to_all(right, "pr", split_axis=2, concat_axis=0, tiled=True),
    )
    strip = jnp.einsum(
        "kid,kjd->ijd",
        lax.all_gather(left_lines, "pc", axis=1, tiled=True),
        right_lines,
        preferred_element_type=F32,
    )
    strip = (strip * count ** (-0.5)).astype(BF16)
    mixed = lax.all_to_all(strip, "pr", split_axis=0, concat_axis=2, tiled=True)
    return to_pair(mixed, ready, mid_gain, out_weight, out_gate)


def nt(a, b):
    return lax.dot_general(a, b, (((1,), (1,)), ((), ())), preferred_element_type=F32)


def tn(a, b):
    return lax.dot_general(a, b, (((0,), (0,)), ((), ())), preferred_element_type=F32)


def kernel(
    n_p, n_q, x_hbm, lw_hbm, rw_hbm, lg_hbm, rg_hbm, gain_hbm, ow_hbm, og_hbm, out_ref,
    x_ref, lw_ref, rw_ref, lg_ref, rg_ref, gain_ref, ow_ref, og_ref, in_s,
    turn, lsend, rsend, lrecv, rrecv, osend, orecv, gate,
    l_ss, l_rs, r_ss, r_rs, lf_ss, lf_rs, rf_ss, rf_rs, o_ss, o_rs,
):
    p = lax.axis_index("pr")
    q = lax.axis_index("pc")
    half = q // 2
    is_inner = lax.rem(half + q, 2) == 1
    inner, end = 1 + half, 3 * half
    partner = half * 2 + 1 - lax.rem(q, 2)
    across = 2 - half
    other_end = 3 - end
    per = lsend.shape[1] // SUB
    width = x_ref.shape[1]
    rows = x_ref.shape[0] // 2
    channels = n_p * per
    count = n_p * x_ref.shape[0]

    def peer(m):
        bits, to, scale = m, 0, 1
        while scale < n_p:
            to = to + lax.rem(p // scale + bits % 2, 2) * scale
            bits, scale = bits // 2, scale * 2
        return to

    brought = [
        pltpu.make_async_copy(src, dst, in_s.at[at])
        for at, (src, dst) in enumerate(
            (
                (x_hbm, x_ref), (rw_hbm, rw_ref), (rg_hbm, rg_ref), (lw_hbm, lw_ref),
                (lg_hbm, lg_ref), (og_hbm, og_ref), (ow_hbm, ow_ref), (gain_hbm, gain_ref),
            )
        )
    ]
    for copy in brought:
        copy.start()

    barrier = pltpu.get_barrier_semaphore()
    for m in range(n_p):
        for dq in range(n_q):
            if (m, dq) != (0, 0):
                to = (peer(m), lax.rem(q + dq, n_q))
                pl.semaphore_signal(barrier, inc=1, device_id=to, device_id_type=MESH)

    def pair_rows(k):
        return jnp.concatenate([x_ref[k], x_ref[k + rows]], axis=0)

    def factor(w_ref, g_ref, send):
        both = jnp.concatenate([w_ref[...].T, g_ref[...].T], axis=0)

        def step(k, _):
            pr = nt(both, pair_rows(k))
            turn[pl.ds(k, channels, stride=SUB), :] = pr[:channels] * jax.nn.sigmoid(pr[channels:])
            return 0

        lax.fori_loop(0, rows, step, 0, unroll=UF)

        def cast(e, _):
            at = pl.multiple_of(e * per * SUB, per * SUB)
            send[e] = turn[pl.ds(at, per * SUB), :].astype(BF16)
            return 0

        lax.fori_loop(0, n_p, cast, 0, unroll=4)

    def remote(src, dst, ss, rs, to):
        return pltpu.make_async_remote_copy(
            src_ref=src, dst_ref=dst, send_sem=ss, recv_sem=rs, device_id=to, device_id_type=MESH
        )

    def r_copy(m):
        to = peer(m)
        return remote(rsend.at[to], rrecv.at[0, m], r_ss.at[m], r_rs.at[m], (to, q))

    def l_copy(m):
        to = peer(m)
        return remote(lsend.at[to], lrecv.at[0, m], l_ss.at[m], l_rs.at[m], (to, q))

    def r_forward(m):
        src = rsend.at[p] if m == 0 else rrecv.at[0, m]
        return remote(src, rrecv.at[1, m], rf_ss.at[m], rf_rs.at[m], (p, partner))

    mine = jnp.where(is_inner, 0, 1)

    def l_forward(m):
        src = lsend.at[p] if m == 0 else lrecv.at[0, m]
        return remote(
            src, lrecv.at[1 + mine, m], lf_ss.at[m], lf_rs.at[mine, m], (p, across)
        )

    def l_arrival(slot, m):
        return remote(
            lsend.at[p], lrecv.at[1 + slot, m], lf_ss.at[m], lf_rs.at[slot, m], (p, across)
        )

    for copy in brought:
        copy.wait()
    factor(rw_ref, rg_ref, rsend)
    pl.semaphore_wait(barrier, n_p * n_q - 1)
    r_forward(0).start()
    for m in range(1, n_p):
        r_copy(m).start()
    factor(lw_ref, lg_ref, lsend)

    @pl.when(is_inner)
    def _():
        l_forward(0).start()

    for m in range(1, n_p):
        l_copy(m).start()
    rrecv[0, 0] = rsend[p]
    lrecv[0, 0] = lsend[p]

    def make_gate(k, _):
        gate[k] = jax.nn.sigmoid(
            jnp.dot(pair_rows(k), og_ref[...], preferred_element_type=F32)
        )
        return 0

    for m in range(1, n_p):
        r_copy(m).wait_recv()
        r_forward(m).start()
        l_copy(m).wait_recv()

        @pl.when(is_inner)
        def _():
            l_forward(m).start()

    @pl.when(jnp.logical_not(is_inner))
    def _():
        for m in range(n_p):
            l_forward(m).start()

    lax.fori_loop(0, rows, make_gate, 0, unroll=4)
    for m in range(n_p):
        r_forward(m).wait_recv()

    low = lax.broadcasted_iota(jnp.int32, (SUB, LANES), 1) < width

    def o_copy(group, z, b, dl):
        to_p = z * 2 + b
        away = (to_p != p) if dl == 0 else None
        return away, remote(
            osend.at[group, b, dl], orecv.at[p], o_ss.at[group, b, dl], o_rs.at[p],
            (to_p, partner if dl else q),
        )

    def run_group(group, z):
        def products(d, _):
            at = pl.ds(pl.multiple_of(d * SUB, SUB), SUB)
            left = lrecv[group, :, at, :].reshape(n_p * SUB, LANES)
            right = [rrecv[dl, :, at, :].reshape(n_p * SUB, LANES) for dl in range(2)]
            sums = tn(left, jnp.concatenate(right, axis=1))
            for dl in range(2):
                acc = sums[:, dl * LANES : (dl + 1) * LANES]
                for b in range(2):
                    top = b * 2 * SUB
                    a0, c0 = acc[top : top + SUB], acc[top + SUB : top + 2 * SUB]
                    b0 = acc[width + top : width + top + SUB]
                    d0 = acc[width + top + SUB : width + top + 2 * SUB]
                    tile = jnp.where(low, a0, d0) + pltpu.roll(
                        jnp.where(low, c0, b0), width, 1
                    )
                    osend[group, b, dl, at, :] = (tile * count ** (-0.5)).astype(BF16)
            return 0

        lax.fori_loop(0, per, products, 0, unroll=UP)
        for dl in (1, 0):
            for b in range(2):
                away, copy = o_copy(group, z, b, dl)
                if away is None:
                    copy.start()
                else:

                    @pl.when(away)
                    def _():
                        copy.start()

                    @pl.when(jnp.logical_not(away))
                    def _():
                        orecv[p] = osend[group, b, dl]

    def end_group(group, z):
        for b in range(2):
            for dl in range(2):
                away, copy = o_copy(group, z, b, dl)
                if away is None:
                    copy.wait_send()
                else:

                    @pl.when(away)
                    def _():
                        copy.wait_send()

    far = ((1, 3 - q), (2, other_end))
    run_group(0, q)

    @pl.when(is_inner)
    def _():
        for slot, (group, z) in enumerate(far):
            for m in range(n_p):
                l_arrival(slot, m).wait_recv()
            run_group(group, z)

    gain = jnp.broadcast_to(gain_ref[...], (channels, channels)).T

    def o_arrival(at):
        return remote(
            osend.at[0, 0, 1], orecv.at[at], o_ss.at[0, 0, 1], o_rs.at[at], (p, partner)
        )

    for m in range(1, n_p):
        o_arrival(peer(m)).wait_recv()
    source = jnp.where(p // 2 == end, end, inner)

    @pl.when(source != q)
    def _():
        o_arrival(p).wait_recv()

    def widen(e, _):
        at = pl.multiple_of(e * per * SUB, per * SUB)
        turn[pl.ds(at, per * SUB), :] = orecv[e].astype(F32)
        return 0

    lax.fori_loop(0, n_p, widen, 0, unroll=4)

    def finish(k, _):
        v = turn[pl.ds(k, channels, stride=SUB), :]
        v = v - jnp.mean(v, axis=0, keepdims=True)
        v = v * lax.rsqrt(jnp.mean(v * v, axis=0, keepdims=True) + 1e-05) * gain
        res = (tn(v.astype(BF16), ow_ref[...]) * gate[k]).astype(BF16)
        out_ref[k] = res[:width]
        out_ref[k + rows] = res[width:]
        return 0

    lax.fori_loop(0, rows, finish, 0, unroll=UE)

    for m in range(n_p):
        if m > 0:
            r_copy(m).wait_send()
            l_copy(m).wait_send()
        r_forward(m).wait_send()
        l_forward(m).wait_send()
    end_group(0, q)

    @pl.when(is_inner)
    def _():
        for group, z in far:
            end_group(group, z)


def fused(n_p, n_q, pair_array, lw, rw, lg, rg, gain, ow, og):
    channels = lw.shape[1]
    slab = channels // n_p * SUB
    rows = pair_array.shape[0] // 2
    dma = pltpu.SemaphoreType.DMA
    return pl.pallas_call(
        functools.partial(kernel, n_p, n_q),
        out_shape=jax.ShapeDtypeStruct(pair_array.shape, BF16),
        in_specs=[pl.BlockSpec(memory_space=pltpu.HBM)] * 8,
        out_specs=pl.BlockSpec(memory_space=pltpu.VMEM),
        scratch_shapes=[
            pltpu.VMEM(pair_array.shape, BF16),
            *[pltpu.VMEM(lw.shape, BF16)] * 4,
            pltpu.VMEM((1, channels), F32),
            pltpu.VMEM(ow.shape, BF16),
            pltpu.VMEM(og.shape, BF16),
            dma((8,)),
            pltpu.VMEM((channels * SUB, LANES), F32),
            pltpu.VMEM((n_p, slab, LANES), BF16),
            pltpu.VMEM((n_p, slab, LANES), BF16),
            pltpu.VMEM((3, n_p, slab, LANES), BF16),
            pltpu.VMEM((2, n_p, slab, LANES), BF16),
            pltpu.VMEM((3, 2, 2, slab, LANES), BF16),
            pltpu.VMEM((n_p, slab, LANES), BF16),
            pltpu.VMEM((rows, LANES, channels), F32),
            *[dma((n_p,))] * 5,
            dma((2, n_p)),
            *[dma((n_p,))] * 2,
            dma((3, 2, 2)),
            dma((n_p,)),
        ],
        compiler_params=pltpu.CompilerParams(
            collective_id=0, has_side_effects=True, vmem_limit_bytes=67_043_328
        ),
    )(pair_array, lw, rw, lg, rg, gain.reshape(1, channels), ow, og)


def solution(mesh):
    n_p, n_q = mesh.shape["pr"], mesh.shape["pc"]

    def on_device(pair_array, lw, *rest):
        first, second, wide = pair_array.shape
        fits = (
            n_q == 4
            and first == 2 * SUB
            and second == 2 * first
            and n_p == 2 * n_q
            and 2 * second == LANES
            and wide == LANES
            and lw.shape[1] == LANES
        )
        if fits:
            return fused(n_p, n_q, pair_array, lw, *rest)
        return plain(pair_array, lw, *rest)

    return jax.shard_map(
        on_device,
        mesh=mesh,
        in_specs=(P("pr", "pc", None), P(), P(), P(), P(), P(), P(), P()),
        out_specs=P("pr", "pc", None),
        check_vma=False,
    )
```
